128 devices in a mesh: row: 16 (over y, z), col: 8 (over x, core).
Axes of the slice: x: 4, y: 4, z: 4, core: 2. Of those that a mesh axis runs over, the one named last changes fastest.
Arguments:
- new_dosage: float32 [8192, 1024], P(('col', 'row')), may hold values from 0 to 2
- old_dosage: float32 [32768, 1024], P(('row', 'col')), may hold values from 0 to 2
- grm: bfloat16 [32768, 8192], P('row', 'col'), may hold values from -1.5 to 1.5
- counts: int32 [16], P('col'), may hold values from 256 to 512
- affected: int32 [64, 16], P('row', 'col'), may hold values from 0 to 1, as said below
Outputs:
- updated: bfloat16 [32768, 8192], P('row', 'col')
The draws below stay inside these ranges and needn't reach their ends.
Inputs may be any that keep to these rules, and one draw needn't show every extreme that they name: `affected`: the density of marked tile pairs differs from one tile of new samples to the next.
All inputs are finite; a program needn't handle non-finite values.
Results may differ from the reference program's by a relative error of at most 0.00115.
Values may be sent and summed in bfloat16 or wider, within the bound.
A program may use at most 128 MiB of HBM per device.

```python
import jax
import jax.numpy as jnp
from jax import lax

SNP = 1024
TILE = 512
REF_DEV = 2048
ALL = 32768
NEW = 8192
N_ROW = 16


def frequency_table(key):
    base_key, shift_key = jax.random.split(jax.random.fold_in(key, 5))
    base_rate = jax.random.uniform(base_key, (1, SNP), jnp.float32, 0.2, 0.8)
    shift_table = jax.random.uniform(shift_key, (16, SNP), jnp.float32, -0.15, 0.15)
    return base_rate + shift_table


def dosage_common(key, own_key, sample_count):
    frequency = frequency_table(key)
    subkeys = jax.random.split(own_key, 4)
    population = jax.random.randint(subkeys[0], (sample_count,), 0, 16)
    jitter = jax.random.uniform(subkeys[1], (sample_count, 1), jnp.float32, -0.02, 0.02)
    chance = jnp.clip(frequency[population] + jitter, 0.03, 0.97)
    allele_draw = jax.random.uniform(subkeys[2], (sample_count, SNP), jnp.float32, 0.0, 1.0)
    absent = (1.0 - chance) * (1.0 - chance)
    called = (allele_draw > absent).astype(jnp.float32) + (allele_draw > 1.0 - chance * chance).astype(jnp.float32)
    weight_draw = jax.random.uniform(subkeys[3], (sample_count, SNP), jnp.float32, 0.0, 1.0)
    shrinkage = 0.3 * weight_draw
    dosage = (1.0 - shrinkage) * called + shrinkage * 2.0 * chance
    return jnp.clip(dosage, 0.0, 2.0).astype(jnp.float32)


def draw_new_dosage(key, part):
    return dosage_common(key, jax.random.fold_in(key, 11), NEW)


def draw_old_dosage(key, part):
    return dosage_common(key, jax.random.fold_in(key, 23), ALL)


def draw_affected(key, part):
    first_key, second_key = jax.random.split(jax.random.fold_in(key, 37))
    offset = jax.random.randint(first_key, (), 0, 4)
    density = 1 + (jnp.arange(NEW // TILE) + offset) % 4
    tickets = jax.random.randint(second_key, (ALL // TILE, NEW // TILE), 0, 4)
    return (tickets < density[None, :]).astype(jnp.int32)


def touch_ends(drawn, key, least, top_value):
    dims = drawn.shape
    place = [jax.random.randint(jax.random.fold_in(key, axis), (), 0, dims[axis]) for axis in range(len(dims))]
    drawn = drawn.at[tuple(place)].set(least)
    longest = dims.index(max(dims))
    place[longest] = (place[longest] + 1) % dims[longest]
    return drawn.at[tuple(place)].set(top_value)


def level_of(key, shape, pieces, low, high):
    factor_of = 1.0
    for position, shards_of in pieces:
        draws = jax.random.uniform(jax.random.fold_in(jax.random.fold_in(key, 6), position), (shards_of,), jnp.float32, low / len(pieces), high / len(pieces))
        factor_of = factor_of * jnp.repeat(jnp.exp(draws), shape[position] // shards_of).reshape((-1,) + (1,) * (len(shape) - 1 - position))
    return factor_of


def gaussian(rng, shape, width, bound, cuts=(), held_as=jnp.bfloat16):
    values = width * jax.random.normal(rng, shape, jnp.float32)
    if cuts:
        values = values * level_of(rng, shape, cuts, -0.22, 0.18)
    return jnp.clip(values, -bound, bound).astype(held_as)


def setup_inputs(seed: int = 0) -> dict:
    arg_keys = jax.random.split(jax.random.key(seed), 6)
    new_dosage = draw_new_dosage(jax.random.fold_in(arg_keys[5], 71), 0)
    old_dosage = draw_old_dosage(jax.random.fold_in(arg_keys[5], 71), 0)
    grm = gaussian(arg_keys[2], (ALL, NEW), 0.1, 1.5, ((0, 16), (1, 8)))
    counts = touch_ends(jax.random.randint(arg_keys[3], (NEW // TILE,), TILE // 2, TILE + 1), jax.random.fold_in(arg_keys[3], 1), TILE // 2, TILE).astype(jnp.int32)
    affected = draw_affected(jax.random.fold_in(arg_keys[5], 71), 0)
    return {"new_dosage": new_dosage, "old_dosage": old_dosage, "grm": grm, "counts": counts, "affected": affected}


def reference(new_dosage, old_dosage, grm, counts, affected):
    totals = lax.optimization_barrier(jnp.sum(old_dosage, axis=0))
    doubled = totals / ALL
    spread = jnp.sqrt(doubled * (1.0 - 0.5 * doubled) + 0.1)
    usable = (jnp.arange(TILE)[None, :] < counts[:, None]).reshape(NEW).astype(jnp.float32)
    new_scores = ((new_dosage - doubled) / spread * usable[:, None]).astype(jnp.bfloat16)
    old_scores = ((old_dosage - doubled) / spread).astype(jnp.bfloat16)
    new_wide = new_scores.astype(jnp.float32)
    old_blocks = old_scores.reshape(N_ROW, REF_DEV, SNP)
    grm_blocks = grm.reshape(N_ROW, REF_DEV, NEW)
    mark_blocks = affected.reshape(N_ROW, REF_DEV // TILE, NEW // TILE)

    def update_block(operands):
        scores, grm_block, markers = operands
        product = jnp.dot(scores.astype(jnp.float32), new_wide.T, precision=lax.Precision.HIGHEST) / SNP
        spread_marks = jnp.repeat(jnp.repeat(markers.astype(jnp.float32), TILE, axis=0), TILE, axis=1)
        return (grm_block.astype(jnp.float32) + product * spread_marks).astype(jnp.bfloat16)
    updated = lax.map(update_block, (old_blocks, grm_blocks, mark_blocks))
    return updated.reshape(ALL, NEW)
```

```python
import functools

import jax
import jax.numpy as jnp
from jax import lax
from jax.experimental import pallas as pl
from jax.experimental.pallas import tpu as pltpu
from jax.sharding import PartitionSpec as P

MESH = pl.DeviceIdType.MESH
TILE = 512
SNP = 1024
RING = 4
CHUNKS = 4


def kernel(
    all_samples,
    old_hbm,
    new_hbm,
    grm_hbm,
    counts,
    affected,
    out,
    old_v,
    new_v,
    grm_v,
    a_v,
    b_v,
    mine1,
    mine2,
    s1,
    s2,
    load_sem,
    s1_send,
    s1_recv,
    s2_send,
    s2_recv,
    a_send,
    a_recv,
    b_send,
    b_recv,
):
    r = lax.axis_index("row")
    c = lax.axis_index("col")
    y, z = r // RING, r % RING
    x, core = c // 2, c % 2
    old_rows, new_rows = old_v.shape[0], new_v.shape[0]
    chunk = old_rows // CHUNKS
    unit = new_rows // 4

    load_old = pltpu.make_async_copy(old_hbm, old_v, load_sem.at[0])
    load_new = pltpu.make_async_copy(new_hbm, new_v, load_sem.at[1])
    load_grm = pltpu.make_async_copy(grm_hbm, grm_v, load_sem.at[2])
    load_old.start()
    load_new.start()
    barrier = pltpu.get_barrier_semaphore()
    for d in range(1, 8):
        pl.semaphore_signal(
            barrier, inc=1, device_id={"col": (c + d) % 8}, device_id_type=MESH
        )
    for d in range(1, 16):
        pl.semaphore_signal(
            barrier, inc=1, device_id={"row": (r + d) % 16}, device_id_type=MESH
        )
    load_grm.start()
    load_old.wait()
    mine1[...] = jnp.sum(old_v[...], axis=0, keepdims=True)
    pl.semaphore_wait(barrier, 22)

    def exchange(axis, me, size, mine, slots, send, recv):
        copies = []
        for d in range(1, size):
            copy = pltpu.make_async_remote_copy(
                src_ref=mine,
                dst_ref=slots.at[d],
                send_sem=send.at[d],
                recv_sem=recv.at[d],
                device_id={axis: (me + d) % size},
                device_id_type=MESH,
            )
            copy.start()
            copies.append(copy)
        total = mine[...]
        for d in range(1, size):
            copies[d - 1].wait_recv()
            total = total + slots[d]
        return total, copies

    total, copies1 = exchange("col", c, 8, mine1, s1, s1_send, s1_recv)
    mine2[...] = total
    total, copies2 = exchange("row", r, 16, mine2, s2, s2_send, s2_recv)
    doubled = total / all_samples
    inverse = 1.0 / jnp.sqrt(doubled * (1.0 - 0.5 * doubled) + 0.1)

    load_new.wait()
    position = (r % 8) * new_rows + lax.broadcasted_iota(jnp.int32, (new_rows, 1), 0)
    usable = (position < counts[0, r // 8]).astype(jnp.float32)
    b_v[pl.ds(pl.multiple_of(r * new_rows, new_rows), new_rows), :] = (
        (new_v[...] - doubled) * inverse * usable
    ).astype(jnp.bfloat16)

    sent = list(copies1) + list(copies2)
    b_index, a_index = {}, {}

    def send_to(ref, sends, recvs, index, key, device):
        slot = index.setdefault(key, len(index))
        copy = pltpu.make_async_remote_copy(
            src_ref=ref,
            dst_ref=ref,
            send_sem=sends.at[slot],
            recv_sem=recvs.at[slot],
            device_id=device,
            device_id_type=MESH,
        )
        copy.start()
        sent.append(copy)

    def arrived(ref, sends, recvs, index, key):
        slot = index.setdefault(key, len(index))
        pltpu.make_async_remote_copy(
            src_ref=ref,
            dst_ref=ref,
            send_sem=sends.at[slot],
            recv_sem=recvs.at[slot],
            device_id={"col": c},
            device_id_type=MESH,
        ).wait_recv()

    def b_block(h, df, ds, first, count):
        dy, dz = (ds, df) if h == 0 else (df, ds)
        block = ((y + dy + RING) % RING) * RING + (z + dz + RING) % RING
        start = block * new_rows + (2 * h + first) * unit
        return b_v.at[pl.ds(pl.multiple_of(start, unit), count * unit)]

    def b_device(h, stage, d):
        along_z = (h == 0) == (stage == 1)
        dy, dz = (0, d) if along_z else (d, 0)
        return {"row": ((y + dy + RING) % RING) * RING + (z + dz + RING) % RING}

    def b_send_block(h, stage, df, first=0, count=2, way=None, forward=False):
        for name, d in (("L", 1), ("R", -1)):
            if way in (None, name):
                key = (h, stage, 0 if stage == 1 else df, name + ("2" if forward else ""))
                if forward:
                    place = (-1 if name == "L" else 1)
                    ref = b_block(h, *((place, 0) if stage == 1 else (df, place)), first, count)
                else:
                    ref = b_block(h, *((0, 0) if stage == 1 else (df, 0)), first, count)
                send_to(ref, b_send, b_recv, b_index, key, b_device(h, stage, d))

    def b_arrived(h, stage, df, name):
        key = (h, stage, df, name)
        place = {"L": -1, "R": 1, "L2": -2, "R2": 2}[name]
        first, count = {"L": (0, 2), "R": (0, 2), "L2": (0, 1), "R2": (1, 1)}[name]
        ref = b_block(h, *((place, 0) if stage == 1 else (df, place)), first, count)
        arrived(ref, b_send, b_recv, b_index, key)

    def b_pass(h, stage, df, name):
        b_arrived(h, stage, df, name)
        b_send_block(h, stage, df, 0 if name == "L" else 1, 1, name, True)

    def a_block(dx, other):
        owner = ((x + dx + RING) % RING) * 2 + (1 - core if other else core)
        return owner

    def a_chunk(dx, other, i):
        start = a_block(dx, other) * old_rows + i * chunk
        return a_v.at[pl.ds(pl.multiple_of(start, chunk), chunk)]

    def a_to(ref, key, d):
        if d is None:
            device = {"col": x * 2 + 1 - core}
        else:
            device = {"col": ((x + d + RING) % RING) * 2 + core}
        send_to(ref, a_send, a_recv, a_index, key, device)

    def a_pass(name, i):
        dx = {"L": -1, "R": 1, "L2": -2, "R2": 2}[name]
        ref = a_chunk(dx, False, i)
        arrived(ref, a_send, a_recv, a_index, (name, i))
        if name == "L" and i < CHUNKS // 2:
            a_to(ref, ("L2", i), 1)
        if name == "R" and i >= CHUNKS // 2:
            a_to(ref, ("R2", i), -1)
        a_to(ref, ("P", abs(dx) if abs(dx) == 2 else dx, i), None)

    def a_from_partner(dx, i):
        arrived(a_chunk(dx, True, i), a_send, a_recv, a_index, ("P", dx, i))

    for h in (0, 1):
        b_send_block(h, 1, 0)
    half = CHUNKS // 2
    for i in range(CHUNKS):
        a_v[pl.ds(pl.multiple_of(c * old_rows + i * chunk, chunk), chunk), :] = (
            (old_v[pl.ds(i * chunk, chunk), :] - doubled) * inverse
        ).astype(jnp.bfloat16)
    for i in range(CHUNKS):
        a_to(a_chunk(0, False, i), ("L", i), 1)
        j = (i + half) % CHUNKS
        a_to(a_chunk(0, False, j), ("R", j), -1)
    for i in range(CHUNKS):
        a_to(a_chunk(0, False, i), ("P", 0, i), None)
    for h in (0, 1):
        b_send_block(h, 2, 0)
    for name in ("L", "R"):
        for h in (0, 1):
            b_pass(h, 1, 0, name)
    for df in (-1, 1):
        for h in (0, 1):
            b_send_block(h, 2, df)
    a_pass("L", 0)
    a_pass("R", half)
    for h in (0, 1):
        b_arrived(h, 1, 0, "L2")
        b_arrived(h, 1, 0, "R2")
        b_send_block(h, 2, 2)
    for name in ("L", "R"):
        for h in (0, 1):
            b_pass(h, 2, 0, name)
    a_pass("L", 1)
    a_pass("R", half + 1)
    for df in (-1, 1):
        for name in ("L", "R"):
            for h in (0, 1):
                b_pass(h, 2, df, name)
    a_pass("L", 2)
    a_pass("R", 0)
    for name in ("L", "R"):
        for h in (0, 1):
            b_pass(h, 2, 2, name)
    a_pass("L", 3)
    a_pass("R", 1)
    for df in (0, -1, 1, 2):
        for name in ("L2", "R2"):
            for h in (0, 1):
                b_arrived(h, 2, df, name)
    load_grm.wait()

    def update(owner):
        rows = pl.ds(pl.multiple_of(owner * old_rows, old_rows), old_rows)
        for j in range(2):
            columns = pl.ds(j * TILE, TILE)
            product = lax.dot_general(
                a_v[rows, :],
                b_v[columns, :],
                (((1,), (1,)), ((), ())),
                preferred_element_type=jnp.float32,
            )
            scale = affected[owner * old_rows // TILE, j].astype(jnp.float32) * (1.0 / SNP)
            out[rows, columns] = (
                grm_v[rows, columns].astype(jnp.float32) + product * scale
            ).astype(jnp.bfloat16)

    update(a_block(0, False))
    for i in range(CHUNKS):
        a_from_partner(0, i)
    update(a_block(0, True))
    update(a_block(-1, False))
    a_pass("L2", 0)
    a_pass("R2", half)
    for i in range(CHUNKS):
        a_from_partner(-1, i)
    update(a_block(-1, True))
    update(a_block(1, False))
    for i in range(CHUNKS):
        a_from_partner(1, i)
    update(a_block(1, True))
    a_pass("L2", 1)
    a_pass("R2", half + 1)
    update(a_block(2, False))
    for i in range(CHUNKS):
        a_from_partner(2, i)
    update(a_block(2, True))
    for copy in sent:
        copy.wait_send()


def on_device(new_dosage, old_dosage, grm, counts, affected):
    old_rows, snps = old_dosage.shape
    new_rows = new_dosage.shape[0]
    devices = lax.axis_size("row") * lax.axis_size("col")
    vmem, dma = pltpu.VMEM, pltpu.SemaphoreType.DMA
    hbm = pl.BlockSpec(memory_space=pltpu.HBM)
    smem = pl.BlockSpec(memory_space=pltpu.SMEM)
    return pl.pallas_call(
        functools.partial(kernel, float(old_rows * devices)),
        out_shape=jax.ShapeDtypeStruct(grm.shape, grm.dtype),
        in_specs=[hbm, hbm, hbm, smem, smem],
        out_specs=pl.BlockSpec(memory_space=pltpu.VMEM),
        scratch_shapes=[
            vmem((old_rows, snps), jnp.float32),
            vmem((new_rows, snps), jnp.float32),
            vmem(grm.shape, grm.dtype),
            vmem((grm.shape[0], snps), jnp.bfloat16),
            vmem((grm.shape[1], snps), jnp.bfloat16),
            vmem((1, snps), jnp.float32),
            vmem((1, snps), jnp.float32),
            vmem((8, 1, snps), jnp.float32),
            vmem((16, 1, snps), jnp.float32),
            dma((3,)),
            dma((8,)),
            dma((8,)),
            dma((16,)),
            dma((16,)),
            dma((28,)),
            dma((28,)),
            dma((40,)),
            dma((40,)),
        ],
        compiler_params=pltpu.CompilerParams(
            collective_id=0, has_side_effects=True, vmem_limit_bytes=40 * 1024 * 1024
        ),
    )(old_dosage, new_dosage, grm, counts.reshape(1, -1), affected)


def solution(mesh):
    placed = (
        P(("col", "row"), None),
        P(("row", "col"), None),
        P("row", "col"),
        P("col"),
        P("row", "col"),
    )
    return jax.shard_map(
        on_device, mesh=mesh, in_specs=placed, out_specs=P("row", "col"), check_vma=False
    )
```

```python
import functools

import jax
import jax.numpy as jnp
from jax import lax
from jax.experimental import pallas as pl
from jax.experimental.pallas import tpu as pltpu
from jax.sharding import PartitionSpec as P

MESH = pl.DeviceIdType.MESH
TILE = 512
SNP = 1024
RING = 4
CHUNKS = 4


def kernel(
    all_samples,
    old_hbm,
    new_hbm,
    grm_hbm,
    counts_hbm,
    affected_hbm,
    out,
    counts,
    affected,
    old_v,
    new_v,
    grm_v,
    a_v,
    b_v,
    mine1,
    mine2,
    s1,
    s2,
    load_sem,
    s1_send,
    s1_recv,
    s2_send,
    s2_recv,
    a_send,
    a_recv,
    b_send,
    b_recv,
):
    r = lax.axis_index("row")
    c = lax.axis_index("col")
    y, z = r // RING, r % RING
    x, core = c // 2, c % 2
    old_rows, new_rows = old_v.shape[0], new_v.shape[0]
    chunk = old_rows // CHUNKS
    unit = new_rows // 4

    load_old = pltpu.make_async_copy(old_hbm, old_v, load_sem.at[0])
    load_new = pltpu.make_async_copy(new_hbm, new_v, load_sem.at[1])
    load_grm = pltpu.make_async_copy(grm_hbm, grm_v, load_sem.at[2])
    load_old.start()
    load_new.start()
    load_counts = pltpu.make_async_copy(counts_hbm, counts, load_sem.at[3])
    load_affected = pltpu.make_async_copy(affected_hbm, affected, load_sem.at[4])
    load_counts.start()
    load_affected.start()
    barrier = pltpu.get_barrier_semaphore()
    for d in range(1, 8):
        pl.semaphore_signal(
            barrier, inc=1, device_id={"col": (c + d) % 8}, device_id_type=MESH
        )
    for d in range(1, 16):
        pl.semaphore_signal(
            barrier, inc=1, device_id={"row": (r + d) % 16}, device_id_type=MESH
        )
    load_grm.start()
    load_old.wait()
    mine1[...] = jnp.sum(old_v[...], axis=0, keepdims=True)
    pl.semaphore_wait(barrier, 22)

    def exchange(axis, me, size, mine, slots, send, recv):
        copies = []
        for d in range(1, size):
            copy = pltpu.make_async_remote_copy(
                src_ref=mine,
                dst_ref=slots.at[d],
                send_sem=send.at[d],
                recv_sem=recv.at[d],
                device_id={axis: (me + d) % size},
                device_id_type=MESH,
            )
            copy.start()
            copies.append(copy)
        total = mine[...]
        for d in range(1, size):
            copies[d - 1].wait_recv()
            total = total + slots[d]
        return total, copies

    total, copies1 = exchange("col", c, 8, mine1, s1, s1_send, s1_recv)
    mine2[...] = total
    total, copies2 = exchange("row", r, 16, mine2, s2, s2_send, s2_recv)
    doubled = total / all_samples
    inverse = 1.0 / jnp.sqrt(doubled * (1.0 - 0.5 * doubled) + 0.1)

    load_new.wait()
    load_counts.wait()
    load_affected.wait()
    position = (r % 8) * new_rows + lax.broadcasted_iota(jnp.int32, (new_rows, 1), 0)
    usable = (position < counts[0, r // 8]).astype(jnp.float32)
    b_v[pl.ds(pl.multiple_of(r * new_rows, new_rows), new_rows), :] = (
        (new_v[...] - doubled) * inverse * usable
    ).astype(jnp.bfloat16)

    sent = list(copies1) + list(copies2)
    b_index, a_index = {}, {}

    def send_to(ref, sends, recvs, index, key, device):
        slot = index.setdefault(key, len(index))
        copy = pltpu.make_async_remote_copy(
            src_ref=ref,
            dst_ref=ref,
            send_sem=sends.at[slot],
            recv_sem=recvs.at[slot],
            device_id=device,
            device_id_type=MESH,
        )
        copy.start()
        sent.append(copy)

    def arrived(ref, sends, recvs, index, key):
        slot = index.setdefault(key, len(index))
        pltpu.make_async_remote_copy(
            src_ref=ref,
            dst_ref=ref,
            send_sem=sends.at[slot],
            recv_sem=recvs.at[slot],
            device_id={"col": c},
            device_id_type=MESH,
        ).wait_recv()

    def b_block(h, df, ds, first, count):
        dy, dz = (ds, df) if h == 0 else (df, ds)
        block = ((y + dy + RING) % RING) * RING + (z + dz + RING) % RING
        start = block * new_rows + (2 * h + first) * unit
        return b_v.at[pl.ds(pl.multiple_of(start, unit), count * unit)]

    def b_device(h, stage, d):
        along_z = (h == 0) == (stage == 1)
        dy, dz = (0, d) if along_z else (d, 0)
        return {"row": ((y + dy + RING) % RING) * RING + (z + dz + RING) % RING}

    def b_send_block(h, stage, df, first=0, count=2, way=None, forward=False):
        for name, d in (("L", 1), ("R", -1)):
            if way in (None, name):
                key = (h, stage, 0 if stage == 1 else df, name + ("2" if forward else ""))
                if forward:
                    place = (-1 if name == "L" else 1)
                    ref = b_block(h, *((place, 0) if stage == 1 else (df, place)), first, count)
                else:
                    ref = b_block(h, *((0, 0) if stage == 1 else (df, 0)), first, count)
                send_to(ref, b_send, b_recv, b_index, key, b_device(h, stage, d))

    def b_arrived(h, stage, df, name):
        key = (h, stage, df, name)
        place = {"L": -1, "R": 1, "L2": -2, "R2": 2}[name]
        first, count = {"L": (0, 2), "R": (0, 2), "L2": (0, 1), "R2": (1, 1)}[name]
        ref = b_block(h, *((place, 0) if stage == 1 else (df, place)), first, count)
        arrived(ref, b_send, b_recv, b_index, key)

    def b_pass(h, stage, df, name):
        b_arrived(h, stage, df, name)
        b_send_block(h, stage, df, 0 if name == "L" else 1, 1, name, True)

    def a_block(dx, other):
        owner = ((x + dx + RING) % RING) * 2 + (1 - core if other else core)
        return owner

    def a_chunk(dx, other, i):
        start = a_block(dx, other) * old_rows + i * chunk
        return a_v.at[pl.ds(pl.multiple_of(start, chunk), chunk)]

    def a_to(ref, key, d):
        if d is None:
            device = {"col": x * 2 + 1 - core}
        else:
            device = {"col": ((x + d + RING) % RING) * 2 + core}
        send_to(ref, a_send, a_recv, a_index, key, device)

    def a_pass(name, i):
        dx = {"L": -1, "R": 1, "L2": -2, "R2": 2}[name]
        ref = a_chunk(dx, False, i)
        arrived(ref, a_send, a_recv, a_index, (name, i))
        if name == "L" and i < CHUNKS // 2:
            a_to(ref, ("L2", i), 1)
        if name == "R" and i >= CHUNKS // 2:
            a_to(ref, ("R2", i), -1)
        a_to(ref, ("P", abs(dx) if abs(dx) == 2 else dx, i), None)

    def a_from_partner(dx, i):
        arrived(a_chunk(dx, True, i), a_send, a_recv, a_index, ("P", dx, i))

    for h in (0, 1):
        b_send_block(h, 1, 0)
    half = CHUNKS // 2
    for i in range(CHUNKS):
        a_v[pl.ds(pl.multiple_of(c * old_rows + i * chunk, chunk), chunk), :] = (
            (old_v[pl.ds(i * chunk, chunk), :] - doubled) * inverse
        ).astype(jnp.bfloat16)
    for i in range(CHUNKS):
        a_to(a_chunk(0, False, i), ("L", i), 1)
        j = (i + half) % CHUNKS
        a_to(a_chunk(0, False, j), ("R", j), -1)
    for i in range(CHUNKS):
        a_to(a_chunk(0, False, i), ("P", 0, i), None)
    for h in (0, 1):
        b_send_block(h, 2, 0)
    for name in ("L", "R"):
        for h in (0, 1):
            b_pass(h, 1, 0, name)
    for df in (-1, 1):
        for h in (0, 1):
            b_send_block(h, 2, df)
    a_pass("L", 0)
    a_pass("R", half)
    for h in (0, 1):
        b_arrived(h, 1, 0, "L2")
        b_arrived(h, 1, 0, "R2")
        b_send_block(h, 2, 2)
    for name in ("L", "R"):
        for h in (0, 1):
            b_pass(h, 2, 0, name)
    a_pass("L", 1)
    a_pass("R", half + 1)
    for df in (-1, 1):
        for name in ("L", "R"):
            for h in (0, 1):
                b_pass(h, 2, df, name)
    a_pass("L", 2)
    a_pass("R", 0)
    for name in ("L", "R"):
        for h in (0, 1):
            b_pass(h, 2, 2, name)
    a_pass("L", 3)
    a_pass("R", 1)
    for df in (0, -1, 1, 2):
        for name in ("L2", "R2"):
            for h in (0, 1):
                b_arrived(h, 2, df, name)
    load_grm.wait()

    def update(owner):
        rows = pl.ds(pl.multiple_of(owner * old_rows, old_rows), old_rows)
        for j in range(2):
            columns = pl.ds(j * TILE, TILE)
            product = lax.dot_general(
                a_v[rows, :],
                b_v[columns, :],
                (((1,), (1,)), ((), ())),
                preferred_element_type=jnp.float32,
            )
            scale = affected[j, owner * old_rows // TILE].astype(jnp.float32) * (1.0 / SNP)
            out[rows, columns] = (
                grm_v[rows, columns].astype(jnp.float32) + product * scale
            ).astype(jnp.bfloat16)

    update(a_block(0, False))
    for i in range(CHUNKS):
        a_from_partner(0, i)
    update(a_block(0, True))
    update(a_block(-1, False))
    a_pass("L2", 0)
    a_pass("R2", half)
    for i in range(CHUNKS):
        a_from_partner(-1, i)
    update(a_block(-1, True))
    update(a_block(1, False))
    for i in range(CHUNKS):
        a_from_partner(1, i)
    update(a_block(1, True))
    a_pass("L2", 1)
    a_pass("R2", half + 1)
    update(a_block(2, False))
    for i in range(CHUNKS):
        a_from_partner(2, i)
    update(a_block(2, True))
    for copy in sent:
        copy.wait_send()


def on_device(new_dosage, old_dosage, grm, counts, affected):
    old_rows, snps = old_dosage.shape
    new_rows = new_dosage.shape[0]
    devices = lax.axis_size("row") * lax.axis_size("col")
    vmem, dma = pltpu.VMEM, pltpu.SemaphoreType.DMA
    hbm = pl.BlockSpec(memory_space=pltpu.HBM)
    operands = (old_dosage, new_dosage, grm, counts.reshape(1, -1), affected.T)
    return pl.pallas_call(
        functools.partial(kernel, float(old_rows * devices)),
        out_shape=jax.ShapeDtypeStruct(grm.shape, grm.dtype),
        in_specs=[hbm] * len(operands),
        out_specs=pl.BlockSpec(memory_space=pltpu.VMEM),
        scratch_shapes=[
            pltpu.SMEM((1, counts.shape[0]), jnp.int32),
            pltpu.SMEM(affected.shape[::-1], jnp.int32),
            vmem((old_rows, snps), jnp.float32),
            vmem((new_rows, snps), jnp.float32),
            vmem(grm.shape, grm.dtype),
            vmem((grm.shape[0], snps), jnp.bfloat16),
            vmem((grm.shape[1], snps), jnp.bfloat16),
            vmem((1, snps), jnp.float32),
            vmem((1, snps), jnp.float32),
            vmem((8, 1, snps), jnp.float32),
            vmem((16, 1, snps), jnp.float32),
            dma((5,)),
            dma((8,)),
            dma((8,)),
            dma((16,)),
            dma((16,)),
            dma((28,)),
            dma((28,)),
            dma((40,)),
            dma((40,)),
        ],
        compiler_params=pltpu.CompilerParams(
            collective_id=0, has_side_effects=True, vmem_limit_bytes=40 * 1024 * 1024
        ),
    )(*[pltpu.with_memory_space_constraint(operand, pltpu.HBM) for operand in operands])


def solution(mesh):
    placed = (
        P(("col", "row"), None),
        P(("row", "col"), None),
        P("row", "col"),
        P("col"),
        P("row", "col"),
    )
    return jax.shard_map(
        on_device, mesh=mesh, in_specs=placed, out_specs=P("row", "col"), check_vma=False
    )
```

```python
import functools

import jax
import jax.numpy as jnp
from jax import lax
from jax.experimental import pallas as pl
from jax.experimental.pallas import tpu as pltpu
from jax.sharding import PartitionSpec as P

MESH = pl.DeviceIdType.MESH
TILE = 512
SNP = 1024
RING = 4
RAW = 64
CHUNKS = 4
COPIES = 54 + 6 * CHUNKS
PLACE = {"L": -1, "R": 1, "L2": 2, "R2": 2}


def contract(left, right):
    return lax.dot_general(
        left, right, (((1,), (1,)), ((), ())), preferred_element_type=jnp.float32
    )


def gather_kernel(
    all_samples,
    old_hbm,
    new_hbm,
    grm_hbm,
    counts_hbm,
    affected_hbm,
    out,
    b_v,
    a_last,
    scale_last,
    counts,
    affected,
    old_v,
    new_v,
    a_v,
    a_raw,
    b_raw,
    mine1,
    mine2,
    s1,
    s2,
    load_sem,
    s1_send,
    s1_recv,
    s2_send,
    s2_recv,
    send_sem,
    recv_sem,
):
    r = lax.axis_index("row")
    c = lax.axis_index("col")
    y, z = r // RING, r % RING
    x, core = c // 2, c % 2
    old_rows, new_rows = old_v.shape[0], new_v.shape[0]
    chunk = (old_rows - RAW) // CHUNKS
    unit = new_rows // 4
    sent, index = [], {}

    def at_col(dx, flip=False):
        return {"col": ((x + dx + RING) % RING) * 2 + (1 - core if flip else core)}

    def at_row(dy, dz):
        return {"row": ((y + dy + RING) % RING) * RING + (z + dz + RING) % RING}

    def copy_of(source, target, key, device):
        slot = index.setdefault(key, len(index))
        return pltpu.make_async_remote_copy(
            src_ref=source,
            dst_ref=target,
            send_sem=send_sem.at[slot],
            recv_sem=recv_sem.at[slot],
            device_id=device,
            device_id_type=MESH,
        )

    def send(source, target, key, device):
        copy = copy_of(source, target, key, device)
        copy.start()
        sent.append(copy)

    def arrived(target, key):
        copy_of(target, target, key, {"col": c}).wait_recv()

    def rows_of(ref, start, count, step):
        return ref.at[pl.ds(pl.multiple_of(start, step), count)]

    load_old = pltpu.make_async_copy(old_hbm, old_v, load_sem.at[0])
    load_new = pltpu.make_async_copy(new_hbm, new_v, load_sem.at[1])
    load_grm = pltpu.make_async_copy(grm_hbm, out, load_sem.at[2])
    load_counts = pltpu.make_async_copy(counts_hbm, counts, load_sem.at[3])
    load_affected = pltpu.make_async_copy(affected_hbm, affected, load_sem.at[4])
    load_old.start()
    load_new.start()
    load_counts.start()
    load_affected.start()
    barrier = pltpu.get_barrier_semaphore()
    for d in range(1, 8):
        pl.semaphore_signal(
            barrier, inc=1, device_id={"col": (c + d) % 8}, device_id_type=MESH
        )
    for d in range(1, 16):
        pl.semaphore_signal(
            barrier, inc=1, device_id={"row": (r + d) % 16}, device_id_type=MESH
        )
    load_grm.start()
    load_old.wait()
    mine1[...] = jnp.sum(old_v[...], axis=0, keepdims=True)
    load_new.wait()
    pl.semaphore_wait(barrier, 22)

    def exchange(axis, me, size, mine, slots, sends, recvs):
        copies = []
        for d in range(1, size):
            copy = pltpu.make_async_remote_copy(
                src_ref=mine,
                dst_ref=slots.at[d],
                send_sem=sends.at[d],
                recv_sem=recvs.at[d],
                device_id={axis: (me + d) % size},
                device_id_type=MESH,
            )
            copy.start()
            copies.append(copy)
            sent.append(copy)
        return copies

    def added(mine, slots, copies):
        total = mine[...]
        for d, copy in enumerate(copies, 1):
            copy.wait_recv()
            total = total + slots[d]
        return total

    def raw_half(owner, i):
        return a_raw.at[owner, pl.ds(i * (RAW // 2), RAW // 2)]

    def raw_owner(dx, flip=False):
        return at_col(dx, flip)["col"]

    copies1 = exchange("col", c, 8, mine1, s1, s1_send, s1_recv)
    for h in (0, 1):
        source = new_v.at[pl.ds(h * 2 * unit, 2 * unit)]
        for name, d in (("L", 1), ("R", -1)):
            device = at_row(0, d) if h == 0 else at_row(d, 0)
            send(source, b_raw.at[3 * h + (d < 0)], ("b1", h, name), device)
    for i in (0, 1):
        for name, d, j in (("L", 1, i), ("R", -1, 1 - i)):
            source = old_v.at[pl.ds(j * (RAW // 2), RAW // 2)]
            send(source, raw_half(c, j), ("raw", name, j), at_col(d))
    send(old_v.at[pl.ds(0, RAW)], a_raw.at[c], ("rawP", 0), at_col(0, True))
    mine2[...] = added(mine1, s1, copies1)
    copies2 = exchange("row", r, 16, mine2, s2, s2_send, s2_recv)
    for name, d, u in (("L", 1, 0), ("R", -1, 1)):
        for h in (0, 1):
            source = b_raw.at[3 * h + (d < 0)]
            arrived(source, ("b1", h, name))
            device = at_row(0, d) if h == 0 else at_row(d, 0)
            part = pl.ds(u * unit, unit)
            send(source.at[part], b_raw.at[3 * h + 2, part], ("b1", h, name + "2"), device)

    def raw_pass(name, i):
        owner = raw_owner(PLACE[name])
        source = raw_half(owner, i)
        arrived(source, ("raw", name, i))
        if (name, i) == ("L", 0):
            send(source, source, ("raw", "L2", i), at_col(1))
        if (name, i) == ("R", 1):
            send(source, source, ("raw", "R2", i), at_col(-1))
        send(source, source, ("rawP", PLACE[name], i), at_col(0, True))

    raw_pass("L", 0)
    raw_pass("R", 1)
    total = added(mine2, s2, copies2)
    doubled = total / all_samples
    inverse = 1.0 / jnp.sqrt(doubled * (1.0 - 0.5 * doubled) + 0.1)

    def scored(dosage):
        return (dosage - doubled) * inverse

    def a_rows(dx, flip, start, count):
        if dx == 2:
            half = (1 - core if flip else core) * old_rows
            return rows_of(a_last, half + start, count, 16)
        return rows_of(a_v, raw_owner(dx, flip) * old_rows + start, count, 16)

    def a_chunk(dx, flip, i):
        return a_rows(dx, flip, RAW + i * chunk, chunk)

    mine = raw_owner(0)

    def a_send_own(name, d, i):
        chunk_of = a_chunk(0, False, i)
        send(chunk_of, chunk_of, ("a", name, i), at_col(d))

    half = CHUNKS // 2
    for i in range(half):
        for j in (i, i + half):
            a_chunk(0, False, j)[...] = scored(
                old_v[pl.ds(RAW + j * chunk, chunk), :]
            ).astype(jnp.bfloat16)
        a_send_own("L", 1, i)
        a_send_own("R", -1, i + half)
    for i in range(half):
        a_send_own("L", 1, i + half)
        a_send_own("R", -1, i)
    a_rows(0, False, 0, RAW)[...] = scored(old_v[pl.ds(0, RAW), :]).astype(jnp.bfloat16)

    def b_row(h, df, ds):
        dy, dz = (ds, df) if h == 0 else (df, ds)
        return at_row(dy, dz)["row"]

    def b_part(h, df, ds, first=0, count=2):
        start = b_row(h, df, ds) * new_rows + (2 * h + first) * unit
        return rows_of(b_v, start, count * unit, unit)

    load_counts.wait()

    def b_score(h, df, source):
        row = b_row(h, df, 0)
        first = (row % 8) * new_rows + 2 * h * unit
        position = first + lax.broadcasted_iota(jnp.int32, (2 * unit, 1), 0)
        usable = (position < counts[0, row // 8]).astype(jnp.float32)
        b_part(h, df, 0)[...] = (scored(source[...]) * usable).astype(jnp.bfloat16)
        for name, d in (("L", 1), ("R", -1)):
            device = at_row(d, 0) if h == 0 else at_row(0, d)
            send(b_part(h, df, 0), b_part(h, df, 0), ("b2", h, df, name), device)

    for h in (0, 1):
        b_score(h, 0, new_v.at[pl.ds(h * 2 * unit, 2 * unit)])
    for df in (-1, 1):
        for h in (0, 1):
            b_score(h, df, b_raw.at[3 * h + (df > 0)])
    for h in (0, 1):
        for name, u in (("L2", 0), ("R2", 1)):
            arrived(b_raw.at[3 * h + 2, pl.ds(u * unit, unit)], ("b1", h, name))
        b_score(h, 2, b_raw.at[3 * h + 2])

    def b_pass(df):
        for name, d, u in (("L", 1, 0), ("R", -1, 1)):
            for h in (0, 1):
                arrived(b_part(h, df, PLACE[name]), ("b2", h, df, name))
                source = b_part(h, df, PLACE[name], u, 1)
                device = at_row(d, 0) if h == 0 else at_row(0, d)
                send(source, source, ("b2", h, df, name + "2"), device)

    def a_pass(name, i):
        dx = PLACE[name]
        source = a_chunk(dx, False, i)
        arrived(source, ("a", name, i))
        if name == "L" and i < half:
            send(source, rows_of(a_last, core * old_rows + RAW + i * chunk, chunk, 16), ("a", "L2", i), at_col(1))
        if name == "R" and i >= half:
            send(source, rows_of(a_last, core * old_rows + RAW + i * chunk, chunk, 16), ("a", "R2", i), at_col(-1))
        send(source, source, ("aP", dx, i), at_col(0, True))

    def raw_scored(dx, flip):
        a_rows(dx, flip, 0, RAW)[...] = scored(a_raw[raw_owner(dx, flip)]).astype(jnp.bfloat16)

    own_part = a_rows(0, False, RAW, old_rows - RAW)
    send(own_part, own_part, ("aP", 0), at_col(0, True))
    raw_pass("L", 1)
    raw_pass("R", 0)
    arrived(a_raw.at[raw_owner(0, True)], ("rawP", 0))
    raw_scored(0, True)
    raw_scored(-1, False)
    raw_scored(1, False)
    raw_pass("L2", 0)
    raw_pass("R2", 1)
    b_pass(0)
    a_pass("L", 0)
    a_pass("R", half)
    b_pass(-1)
    a_pass("L", 1)
    a_pass("R", half + 1)
    b_pass(1)
    raw_scored(2, False)
    for dx in (-1, 1, 2):
        for i in (0, 1):
            arrived(raw_half(raw_owner(dx, True), i), ("rawP", dx, i))
        raw_scored(dx, True)
    for i in range(half):
        a_pass("L", half + i)
        a_pass("R", i)
        if i == 0:
            b_pass(2)
    load_affected.wait()
    last_tile = (x + 2) % RING
    for j in range(2):
        scale_last[:, pl.ds(j * TILE, TILE)] = jnp.full(
            (8, TILE), affected[j, last_tile].astype(jnp.float32) * (1.0 / SNP)
        )
    for df in (0, -1, 1, 2):
        for name, u, place in (("L2", 0, -2), ("R2", 1, 2)):
            for h in (0, 1):
                arrived(b_part(h, df, place, u, 1), ("b2", h, df, name))
    load_grm.wait()

    def update(dx, flip):
        owner = raw_owner(dx, flip)
        rows = pl.ds(pl.multiple_of(owner * old_rows, old_rows), old_rows)
        for j in range(2):
            columns = pl.ds(j * TILE, TILE)
            product = contract(a_v[rows, :], b_v[columns, :])
            scale = affected[j, owner * old_rows // TILE].astype(jnp.float32) * (1.0 / SNP)
            out[rows, columns] = (
                out[rows, columns].astype(jnp.float32) + product * scale
            ).astype(jnp.bfloat16)

    update(0, False)
    own_other = a_rows(0, True, RAW, old_rows - RAW)
    arrived(own_other, ("aP", 0))
    update(0, True)
    update(-1, False)
    for i in range(half):
        if i < half - 1:
            a_pass("L2", i)
            a_pass("R2", half + i)
    update(1, False)
    for dx in (-1, 1):
        for i in range(CHUNKS):
            arrived(a_chunk(dx, True, i), ("aP", dx, i))
        update(dx, True)
    a_pass("L2", half - 1)
    a_pass("R2", CHUNKS - 1)
    for i in range(CHUNKS):
        arrived(a_chunk(2, True, i), ("aP", 2, i))
    for copy in sent:
        copy.wait_send()
    assert len(index) == COPIES, len(index)


def finish_kernel(updated, b_v, a_last, scale_last, result, last, store_sem):
    x = lax.axis_index("col") // 2
    rows = a_last.shape[0]
    stores = []

    def store(source, start, count, columns):
        start = pl.multiple_of(start, count)
        copy = pltpu.make_async_copy(
            source, result.at[pl.ds(start, count), columns], store_sem.at[len(stores)]
        )
        copy.start()
        stores.append(copy)

    whole = pl.ds(0, updated.shape[1])
    for d in (0, 1, 3):
        start = ((x + d) % RING) * rows
        store(updated.at[pl.ds(pl.multiple_of(start, rows), rows)], start, rows, whole)
    mine = ((x + 2) % RING) * rows
    piece = rows // 2
    for i in range(2):
        for j in range(2):
            columns = pl.ds(j * TILE, TILE)
            product = contract(a_last[pl.ds(i * piece, piece), :], b_v[columns, :])
            at = pl.ds(pl.multiple_of(mine + i * piece, piece), piece)
            last[pl.ds(i * piece, piece), columns] = (
                updated[at, columns].astype(jnp.float32) + product * scale_last[0:1, columns]
            ).astype(jnp.bfloat16)
            store(last.at[pl.ds(i * piece, piece), columns], mine + i * piece, piece, columns)
    for copy in stores:
        copy.wait()


def on_device(new_dosage, old_dosage, grm, counts, affected):
    old_rows, snps = old_dosage.shape
    new_rows = new_dosage.shape[0]
    devices = lax.axis_size("row") * lax.axis_size("col")
    vmem, dma = pltpu.VMEM, pltpu.SemaphoreType.DMA
    hbm_spec = pl.BlockSpec(memory_space=pltpu.HBM)
    vmem_spec = pl.BlockSpec(memory_space=pltpu.VMEM)
    operands = (old_dosage, new_dosage, grm, counts.reshape(1, -1), affected.T)
    parts = pl.pallas_call(
        functools.partial(gather_kernel, float(old_rows * devices)),
        out_shape=[
            pltpu.VMEM(grm.shape, grm.dtype),
            pltpu.VMEM((grm.shape[1], snps), jnp.bfloat16),
            pltpu.VMEM((2 * old_rows, snps), jnp.bfloat16),
            pltpu.VMEM((8, grm.shape[1]), jnp.float32),
        ],
        in_specs=[hbm_spec] * len(operands),
        out_specs=[vmem_spec] * 4,
        scratch_shapes=[
            pltpu.SMEM((1, counts.shape[0]), jnp.int32),
            pltpu.SMEM(affected.shape[::-1], jnp.int32),
            vmem((old_rows, snps), jnp.float32),
            vmem((new_rows, snps), jnp.float32),
            vmem((grm.shape[0], snps), jnp.bfloat16),
            vmem((8, RAW, snps), jnp.float32),
            vmem((6, new_rows // 2, snps), jnp.float32),
            vmem((1, snps), jnp.float32),
            vmem((1, snps), jnp.float32),
            vmem((8, 1, snps), jnp.float32),
            vmem((16, 1, snps), jnp.float32),
            dma((5,)),
            dma((8,)),
            dma((8,)),
            dma((16,)),
            dma((16,)),
            dma((COPIES,)),
            dma((COPIES,)),
        ],
        compiler_params=pltpu.CompilerParams(
            collective_id=0, has_side_effects=True, vmem_limit_bytes=40 * 1024 * 1024
        ),
        name="gather",
    )(*[pltpu.with_memory_space_constraint(operand, pltpu.HBM) for operand in operands])
    return pl.pallas_call(
        finish_kernel,
        out_shape=jax.ShapeDtypeStruct(grm.shape, grm.dtype),
        in_specs=[vmem_spec] * 4,
        out_specs=hbm_spec,
        scratch_shapes=[vmem((2 * old_rows, grm.shape[1]), grm.dtype), dma((7,))],
        compiler_params=pltpu.CompilerParams(vmem_limit_bytes=16 * 1024 * 1024),
        name="finish",
    )(*[pltpu.with_memory_space_constraint(part, pltpu.VMEM) for part in parts])


def solution(mesh):
    placed = (
        P(("col", "row"), None),
        P(("row", "col"), None),
        P("row", "col"),
        P("col"),
        P("row", "col"),
    )
    return jax.shard_map(
        on_device, mesh=mesh, in_specs=placed, out_specs=P("row", "col"), check_vma=False
    )
```

```python
import functools
import math

import jax
import jax.numpy as jnp
from jax import lax
from jax.experimental import pallas as pl
from jax.experimental.pallas import tpu as pltpu
from jax.sharding import PartitionSpec as P

MESH = pl.DeviceIdType.MESH
TILE = 512
SNP = 1024
RING = 4
RAW = 64
CHUNKS = 4
ARRIVALS = 24 + 3 * CHUNKS
PLACE = {"L": -1, "R": 1, "L2": 2, "R2": 2}


def contract(left, right):
    return lax.dot_general(
        left, right, (((1,), (1,)), ((), ())), preferred_element_type=jnp.float32
    )


def gather_kernel(
    all_samples,
    old_hbm,
    new_hbm,
    grm_hbm,
    counts_hbm,
    affected_hbm,
    out,
    b_v,
    a_last,
    scale_last,
    counts,
    affected,
    old_v,
    new_v,
    a_v,
    a_raw,
    b_raw,
    mine1,
    mine2,
    s1,
    s2,
    load_sem,
    send_sem,
    recv_sem,
):
    r = lax.axis_index("row")
    c = lax.axis_index("col")
    y, z = r // RING, r % RING
    x, core = c // 2, c % 2
    old_rows, new_rows = old_v.shape[0], new_v.shape[0]
    chunk = (old_rows - RAW) // CHUNKS
    unit = new_rows // 4
    index, sent_rows = {}, {}

    def at_col(dx, flip=False):
        return {"col": ((x + dx + RING) % RING) * 2 + (1 - core if flip else core)}

    def at_row(dy, dz):
        return {"row": ((y + dy + RING) % RING) * RING + (z + dz + RING) % RING}

    def copy_of(source, target, key, group, device):
        return pltpu.make_async_remote_copy(
            src_ref=source,
            dst_ref=target,
            send_sem=send_sem.at[group],
            recv_sem=recv_sem.at[index.setdefault(key, len(index))],
            device_id=device,
            device_id_type=MESH,
        )

    def send(source, target, key, device):
        group = {"raw": 0, "rawP": 0, "b1": 0, "b2": 1, "a": 2, "aP": 2}[key[0]]
        copy_of(source, target, key, group, device).start()
        rows = math.prod(source.shape) * source.dtype.itemsize // (2 * SNP)
        sent_rows[group] = sent_rows.get(group, 0) + rows

    def arrived(key, rows):
        target = out.at[pl.ds(0, rows)]
        copy_of(target, target, key, 0, {"col": c}).wait_recv()

    def rows_of(ref, start, count, step):
        return ref.at[pl.ds(pl.multiple_of(start, step), count)]

    load_old = pltpu.make_async_copy(old_hbm, old_v, load_sem.at[0])
    load_new = pltpu.make_async_copy(new_hbm, new_v, load_sem.at[1])
    load_grm = pltpu.make_async_copy(grm_hbm, out, load_sem.at[2])
    load_counts = pltpu.make_async_copy(counts_hbm, counts, load_sem.at[3])
    load_affected = pltpu.make_async_copy(affected_hbm, affected, load_sem.at[4])
    load_old.start()
    load_new.start()
    load_counts.start()
    load_affected.start()
    barrier = pltpu.get_barrier_semaphore()
    for d in range(1, 8):
        pl.semaphore_signal(
            barrier, inc=1, device_id={"col": (c + d) % 8}, device_id_type=MESH
        )
    for d in range(1, 16):
        pl.semaphore_signal(
            barrier, inc=1, device_id={"row": (r + d) % 16}, device_id_type=MESH
        )
    load_grm.start()
    load_old.wait()
    mine1[...] = jnp.sum(old_v[...], axis=0, keepdims=True)
    load_new.wait()
    pl.semaphore_wait(barrier, 22)

    def exchange(axis, me, size, mine, slots, group):
        for d in range(1, size):
            copy_of(mine, slots.at[d], axis, group, {axis: (me + d) % size}).start()

    def exchanged(axis, size, mine, slots, group):
        landed = slots.at[pl.ds(1, size - 1)]
        copy_of(landed, landed, axis, group, {"col": c}).wait_recv()
        total = mine[...]
        for d in range(1, size):
            total = total + slots[d]
        return total

    def raw_half(owner, i):
        return a_raw.at[owner, pl.ds(i * (RAW // 2), RAW // 2)]

    def raw_owner(dx, flip=False):
        return at_col(dx, flip)["col"]

    exchange("col", c, 8, mine1, s1, 3)
    for h in (0, 1):
        source = new_v.at[pl.ds(h * 2 * unit, 2 * unit)]
        for name, d in (("L", 1), ("R", -1)):
            device = at_row(0, d) if h == 0 else at_row(d, 0)
            send(source, b_raw.at[3 * h + (d < 0)], ("b1", name), device)
    for i in (0, 1):
        for name, d, j in (("L", 1, i), ("R", -1, 1 - i)):
            source = old_v.at[pl.ds(j * (RAW // 2), RAW // 2)]
            send(source, raw_half(c, j), ("raw", name, j), at_col(d))
    send(old_v.at[pl.ds(0, RAW)], a_raw.at[c], ("rawP", 0), at_col(0, True))
    mine2[...] = exchanged("col", 8, mine1, s1, 3)
    exchange("row", r, 16, mine2, s2, 4)
    for name, d, u in (("L", 1, 0), ("R", -1, 1)):
        arrived(("b1", name), 8 * unit)
        for h in (0, 1):
            source = b_raw.at[3 * h + (d < 0)]
            device = at_row(0, d) if h == 0 else at_row(d, 0)
            part = pl.ds(u * unit, unit)
            send(source.at[part], b_raw.at[3 * h + 2, part], ("b1", "2"), device)

    def raw_pass(name, i):
        owner = raw_owner(PLACE[name])
        source = raw_half(owner, i)
        arrived(("raw", name, i), RAW)
        if (name, i) == ("L", 0):
            send(source, source, ("raw", "L2", i), at_col(1))
        if (name, i) == ("R", 1):
            send(source, source, ("raw", "R2", i), at_col(-1))
        send(source, source, ("rawP", PLACE[name]), at_col(0, True))

    raw_pass("L", 0)
    raw_pass("R", 1)
    total = exchanged("row", 16, mine2, s2, 4)
    doubled = total / all_samples
    inverse = 1.0 / jnp.sqrt(doubled * (1.0 - 0.5 * doubled) + 0.1)

    def scored(dosage):
        return (dosage - doubled) * inverse

    def a_rows(dx, flip, start, count):
        if dx == 2:
            half = (1 - core if flip else core) * old_rows
            return rows_of(a_last, half + start, count, 16)
        return rows_of(a_v, raw_owner(dx, flip) * old_rows + start, count, 16)

    def a_chunk(dx, flip, i):
        return a_rows(dx, flip, RAW + i * chunk, chunk)

    mine = raw_owner(0)

    def a_send_own(name, d, i):
        chunk_of = a_chunk(0, False, i)
        send(chunk_of, chunk_of, ("a", name, i), at_col(d))

    half = CHUNKS // 2
    for i in range(half):
        for j in (i, i + half):
            a_chunk(0, False, j)[...] = scored(
                old_v[pl.ds(RAW + j * chunk, chunk), :]
            ).astype(jnp.bfloat16)
        a_send_own("L", 1, i)
        a_send_own("R", -1, i + half)
    for i in range(half):
        a_send_own("L", 1, i + half)
        a_send_own("R", -1, i)
    a_rows(0, False, 0, RAW)[...] = scored(old_v[pl.ds(0, RAW), :]).astype(jnp.bfloat16)

    def b_row(h, df, ds):
        dy, dz = (ds, df) if h == 0 else (df, ds)
        return at_row(dy, dz)["row"]

    def b_part(h, df, ds, first=0, count=2):
        start = b_row(h, df, ds) * new_rows + (2 * h + first) * unit
        return rows_of(b_v, start, count * unit, unit)

    load_counts.wait()

    def b_score(h, df, source):
        row = b_row(h, df, 0)
        first = (row % 8) * new_rows + 2 * h * unit
        position = first + lax.broadcasted_iota(jnp.int32, (2 * unit, 1), 0)
        usable = (position < counts[0, row // 8]).astype(jnp.float32)
        b_part(h, df, 0)[...] = (scored(source[...]) * usable).astype(jnp.bfloat16)
        for name, d in (("L", 1), ("R", -1)):
            device = at_row(d, 0) if h == 0 else at_row(0, d)
            send(b_part(h, df, 0), b_part(h, df, 0), ("b2", df), device)

    for h in (0, 1):
        b_score(h, 0, new_v.at[pl.ds(h * 2 * unit, 2 * unit)])
    for df in (-1, 1):
        for h in (0, 1):
            b_score(h, df, b_raw.at[3 * h + (df > 0)])
    arrived(("b1", "2"), 8 * unit)
    for h in (0, 1):
        b_score(h, 2, b_raw.at[3 * h + 2])

    def b_pass(df):
        arrived(("b2", df), 8 * unit)
        for name, d, u in (("L", 1, 0), ("R", -1, 1)):
            for h in (0, 1):
                source = b_part(h, df, PLACE[name], u, 1)
                device = at_row(d, 0) if h == 0 else at_row(0, d)
                send(source, source, ("b2", "2"), device)

    def a_pass(name, i):
        dx = PLACE[name]
        source = a_chunk(dx, False, i)
        arrived(("a", name, i), chunk)
        if name == "L" and i < half:
            send(source, rows_of(a_last, core * old_rows + RAW + i * chunk, chunk, 16), ("a", "L2", i), at_col(1))
        if name == "R" and i >= half:
            send(source, rows_of(a_last, core * old_rows + RAW + i * chunk, chunk, 16), ("a", "R2", i), at_col(-1))
        send(source, source, ("aP", dx), at_col(0, True))

    def raw_scored(dx, flip):
        a_rows(dx, flip, 0, RAW)[...] = scored(a_raw[raw_owner(dx, flip)]).astype(jnp.bfloat16)

    own_part = a_rows(0, False, RAW, old_rows - RAW)
    send(own_part, own_part, ("aP", 0), at_col(0, True))
    raw_pass("L", 1)
    raw_pass("R", 0)
    arrived(("rawP", 0), 2 * RAW)
    raw_scored(0, True)
    raw_scored(-1, False)
    raw_scored(1, False)
    raw_pass("L2", 0)
    raw_pass("R2", 1)
    b_pass(0)
    b_pass(-1)
    a_pass("L", 0)
    a_pass("R", half)
    b_pass(1)
    b_pass(2)
    raw_scored(2, False)
    for dx in (-1, 1, 2):
        arrived(("rawP", dx), 2 * RAW)
        raw_scored(dx, True)
    load_affected.wait()
    last_tile = (x + 2) % RING
    for j in range(2):
        scale_last[:, pl.ds(j * TILE, TILE)] = jnp.full(
            (8, TILE), affected[j, last_tile].astype(jnp.float32) * (1.0 / SNP)
        )
    load_grm.wait()
    for i in range(1, half):
        a_pass("L", i)
        a_pass("R", half + i)
    for i in range(half - 1):
        a_pass("L", half + i)
        a_pass("R", i)
    arrived(("b2", "2"), 16 * unit)
    arrived(("aP", 0), old_rows - RAW)

    def update(dx):
        tile = (x + dx + RING) % RING
        rows = pl.ds(pl.multiple_of(tile * TILE, TILE), TILE)
        for j in range(2):
            columns = pl.ds(j * TILE, TILE)
            product = contract(a_v[rows, :], b_v[columns, :])
            scale = affected[j, tile].astype(jnp.float32) * (1.0 / SNP)
            out[rows, columns] = (
                out[rows, columns].astype(jnp.float32) + product * scale
            ).astype(jnp.bfloat16)

    a_pass("L", CHUNKS - 1)
    a_pass("R", half - 1)
    update(0)
    arrived(("aP", -1), old_rows - RAW)
    update(-1)
    for i in range(half):
        a_pass("L2", i)
        a_pass("R2", half + i)
    arrived(("aP", 1), old_rows - RAW)
    update(1)
    arrived(("aP", 2), old_rows - RAW)
    for group, rows in sent_rows.items():
        target = out.at[pl.ds(0, rows)]
        copy_of(target, target, "col", group, {"col": c}).wait_send()
    for axis, size, slots, group in (("col", 8, s1, 3), ("row", 16, s2, 4)):
        landed = slots.at[pl.ds(1, size - 1)]
        copy_of(landed, landed, axis, group, {"col": c}).wait_send()
    assert len(index) == ARRIVALS, len(index)


def finish_kernel(updated, b_v, a_last, scale_last, result, last, store_sem):
    x = lax.axis_index("col") // 2
    rows = a_last.shape[0]

    def store(source, start, count, columns):
        start = pl.multiple_of(start, count)
        pltpu.make_async_copy(
            source, result.at[pl.ds(start, count), columns], store_sem
        ).start()

    whole = pl.ds(0, updated.shape[1])
    for d in (0, 1, 3):
        start = ((x + d) % RING) * rows
        store(updated.at[pl.ds(pl.multiple_of(start, rows), rows)], start, rows, whole)
    mine = ((x + 2) % RING) * rows
    piece = rows // 2
    for i in range(2):
        for j in range(2):
            columns = pl.ds(j * TILE, TILE)
            product = contract(a_last[pl.ds(i * piece, piece), :], b_v[columns, :])
            at = pl.ds(pl.multiple_of(mine + i * piece, piece), piece)
            last[pl.ds(i * piece, piece), columns] = (
                updated[at, columns].astype(jnp.float32) + product * scale_last[0:1, columns]
            ).astype(jnp.bfloat16)
            store(last.at[pl.ds(i * piece, piece), columns], mine + i * piece, piece, columns)
    pltpu.make_async_copy(updated, result, store_sem).wait()


def on_device(new_dosage, old_dosage, grm, counts, affected):
    old_rows, snps = old_dosage.shape
    new_rows = new_dosage.shape[0]
    devices = lax.axis_size("row") * lax.axis_size("col")
    vmem, dma = pltpu.VMEM, pltpu.SemaphoreType.DMA
    hbm_spec = pl.BlockSpec(memory_space=pltpu.HBM)
    vmem_spec = pl.BlockSpec(memory_space=pltpu.VMEM)
    operands = (old_dosage, new_dosage, grm, counts.reshape(1, -1), affected.T)
    parts = pl.pallas_call(
        functools.partial(gather_kernel, float(old_rows * devices)),
        out_shape=[
            pltpu.VMEM(grm.shape, grm.dtype),
            pltpu.VMEM((grm.shape[1], snps), jnp.bfloat16),
            pltpu.VMEM((2 * old_rows, snps), jnp.bfloat16),
            pltpu.VMEM((8, grm.shape[1]), jnp.float32),
        ],
        in_specs=[hbm_spec] * len(operands),
        out_specs=[vmem_spec] * 4,
        scratch_shapes=[
            pltpu.SMEM((1, counts.shape[0]), jnp.int32),
            pltpu.SMEM(affected.shape[::-1], jnp.int32),
            vmem((old_rows, snps), jnp.float32),
            vmem((new_rows, snps), jnp.float32),
            vmem((grm.shape[0], snps), jnp.bfloat16),
            vmem((8, RAW, snps), jnp.float32),
            vmem((6, new_rows // 2, snps), jnp.float32),
            vmem((1, snps), jnp.float32),
            vmem((1, snps), jnp.float32),
            vmem((8, 1, snps), jnp.float32),
            vmem((16, 1, snps), jnp.float32),
            dma((5,)),
            dma((5,)),
            dma((ARRIVALS,)),
        ],
        compiler_params=pltpu.CompilerParams(
            collective_id=0, has_side_effects=True, vmem_limit_bytes=40 * 1024 * 1024
        ),
        name="gather",
    )(*[pltpu.with_memory_space_constraint(operand, pltpu.HBM) for operand in operands])
    return pl.pallas_call(
        finish_kernel,
        out_shape=jax.ShapeDtypeStruct(grm.shape, grm.dtype),
        in_specs=[vmem_spec] * 4,
        out_specs=hbm_spec,
        scratch_shapes=[vmem((2 * old_rows, grm.shape[1]), grm.dtype), dma(())],
        compiler_params=pltpu.CompilerParams(vmem_limit_bytes=16 * 1024 * 1024),
        name="finish",
    )(*[pltpu.with_memory_space_constraint(part, pltpu.VMEM) for part in parts])


def solution(mesh):
    placed = (
        P(("col", "row"), None),
        P(("row", "col"), None),
        P("row", "col"),
        P("col"),
        P("row", "col"),
    )
    return jax.shard_map(
        on_device, mesh=mesh, in_specs=placed, out_specs=P("row", "col"), check_vma=False
    )
```
